16 devices in a mesh: row: 2 (over z), col: 8 (over y, x, core).
Axes of the slice: x: 2, y: 2, z: 2, core: 2. Of those that a mesh axis runs over, the one named last changes fastest.
Arguments:
- v_panels: float32 [8192, 8192], P('row', 'col')
- t_factors: float32 [64, 128, 128], P('col')
- z_vecs: float32 [8192, 4096], P(None, ('row', 'col'))
Outputs:
- output: float32 [8192, 4096], P(None, ('row', 'col'))
All inputs are finite; a program needn't handle non-finite values.
Results may differ from the reference program's by a relative error of at most 0.001.
Values sent between devices are 32-bit elements.
A program may use at most 1 GiB of HBM per device.

```python
import jax
import jax.numpy as jnp
from jax import lax

N = 8192
BLOCK = 128
K_DEV = 256
ROW_DEV = 2
COL_DEV = 8

NPANEL = N // BLOCK
M_LOC = NPANEL // COL_DEV
K_COLS = K_DEV * ROW_DEV * COL_DEV


def build_inputs(raw_vals, z_vecs):
    row_nat = jnp.arange(N)[:, None, None]
    diag_row = (jnp.arange(NPANEL) * BLOCK)[None, :, None] + jnp.arange(BLOCK)[None, None, :]
    v_nat = jnp.where(row_nat > diag_row, raw_vals, jnp.where(row_nat == diag_row, 1.0, 0.0)).astype(raw_vals.dtype)
    gram = jnp.einsum("nmb,nmc->mbc", v_nat, v_nat, precision=lax.Precision.HIGHEST)
    half_diag = 0.5 * jnp.diagonal(gram, axis1=1, axis2=2)
    t_inverse = jnp.triu(gram, 1) + jnp.eye(BLOCK, dtype=raw_vals.dtype) * half_diag[:, None, :]
    t_nat = jnp.triu(jnp.linalg.inv(t_inverse))
    v_cols = v_nat.reshape(N, M_LOC, COL_DEV, BLOCK).transpose(0, 2, 1, 3).reshape(N, N)
    v_store = v_cols.reshape(NPANEL // ROW_DEV, ROW_DEV, BLOCK, N).transpose(1, 0, 2, 3).reshape(N, N)
    t_store = t_nat.reshape(M_LOC, COL_DEV, BLOCK, BLOCK).transpose(1, 0, 2, 3).reshape(NPANEL, BLOCK, BLOCK)
    return {"v_panels": v_store, "t_factors": t_store, "z_vecs": z_vecs}


def setup_inputs(seed: int = 0) -> dict:
    base_key = jax.random.key(seed)
    key_v, key_z = jax.random.split(base_key)
    raw_vals = jax.random.normal(key_v, (N, NPANEL, BLOCK), jnp.float32)
    z_vecs = jax.random.normal(key_z, (N, K_COLS), jnp.float32)
    return build_inputs(raw_vals, z_vecs)


def reference(v_panels, t_factors, z_vecs):
    def apply_panel(x_cur, panel_idx):
        store_slot = (panel_idx % COL_DEV) * M_LOC + panel_idx // COL_DEV
        v_blk = lax.dynamic_slice_in_dim(v_panels, store_slot * BLOCK, BLOCK, axis=1)
        t_blk = lax.dynamic_index_in_dim(t_factors, store_slot, axis=0, keepdims=False)
        w_blk = jnp.dot(v_blk.T, x_cur, precision=lax.Precision.HIGHEST, preferred_element_type=jnp.float32)
        y_blk = jnp.dot(t_blk, w_blk, precision=lax.Precision.HIGHEST, preferred_element_type=jnp.float32)
        x_new = x_cur - jnp.dot(v_blk, y_blk, precision=lax.Precision.HIGHEST, preferred_element_type=jnp.float32)
        return x_new, None

    x_out, _ = lax.scan(apply_panel, z_vecs, jnp.arange(NPANEL - 1, -1, -1))
    return x_out
```

```python
import functools
import jax, jax.numpy as jnp
from jax import lax
from jax.experimental import pallas as pl
from jax.experimental.pallas import tpu as pltpu

BF = jnp.bfloat16
F32 = jnp.float32
TN = (((0,), (0,)), ((), ()))
TR = 512

def split3(v):
    h = v.astype(BF)
    r = v - h.astype(F32)
    m = r.astype(BF)
    l = (r - m.astype(F32)).astype(BF)
    return h, m, l

def mm(a, b):
    return jnp.dot(a, b, preferred_element_type=F32)

def mmt(a, b):
    return lax.dot_general(a, b, TN, preferred_element_type=F32)

def stage1(half, off, p, X, VF, C, XS, YC, upd, wacc, src, dst):
    for r in range(2):
        rows = pl.ds(pl.multiple_of(r * half + off, TR), TR)
        x = X[rows, :]
        if upd:
            x = x - (mm(C[src, 0, rows, :], YC[0]) + mm(C[src, 0, rows, :], YC[1]) + mm(C[src, 1, rows, :], YC[2]))
            X[rows, :] = x
        if wacc:
            prow = pl.ds(r * TR, TR)
            xh, xm, xl = split3(x)
            XS[p, 0, prow, :] = xh
            XS[p, 1, prow, :] = xm
            XS[p, 2, prow, :] = xl
            vh, vm, vl = split3(VF[dst, rows, :])
            C[dst, 0, rows, :128] = vh
            C[dst, 0, rows, 128:] = vm
            C[dst, 1, rows, :128] = vh
            C[dst, 1, rows, 128:] = vl

def stage2(half, off, p, C, XS, A, B, dst):
    a = A[...]
    b = B[...]
    for r in range(2):
        rows = pl.ds(pl.multiple_of(r * half + off, TR), TR)
        prow = pl.ds(r * TR, TR)
        n1 = C[dst, 0, rows, :]
        a += mmt(n1, XS[p, 0, prow, :]) + mmt(n1, XS[p, 1, prow, :])
        b += mmt(C[dst, 1, rows, 128:], XS[p, 0, prow, :]) + mmt(n1[:, :128], XS[p, 2, prow, :])
    A[...] = a
    B[...] = b

def make_y(tq, A, B, YC):
    w = A[:128, :] + A[128:, :] + B[...]
    th, tm, tl = split3(tq)
    wh, wm, wl = split3(w)
    t1 = jnp.concatenate([th, tm], axis=1)
    t2 = jnp.concatenate([th, tl], axis=1)
    y = mm(t1, jnp.concatenate([wh, wh], axis=0)) + mm(t1, jnp.concatenate([wm, wm], axis=0)) + mm(t2, jnp.concatenate([wl, wh], axis=0))
    yh, ym, yl = split3(y)
    YC[0] = jnp.concatenate([yh, yh], axis=0)
    YC[1] = jnp.concatenate([ym, ym], axis=0)
    YC[2] = jnp.concatenate([yl, yh], axis=0)
    A[...] = jnp.zeros_like(A)
    B[...] = jnp.zeros_like(B)

def group_kernel(t, vt, tq, x_in, x_out, X, VF, C, XS, YC, A, B, vsem, xsem):
    half = X.shape[0] // 2
    first = t * TR
    n = half - first
    nt = n // TR
    def xcopy(r, inward):
        sl = pl.ds(r * half + first, n)
        if inward:
            return pltpu.make_async_copy(x_in.at[sl, :], X.at[sl, :], xsem.at[r])
        return pltpu.make_async_copy(X.at[sl, :], x_out.at[sl, :], xsem.at[r])
    def vcopy(q, slot, r):
        return pltpu.make_async_copy(vt.at[r * 8 + q], VF.at[slot, pl.ds(r * half + first, n), :], vsem.at[slot, r])
    for r in range(2):
        xcopy(r, True).start()
        vcopy(7, 1, r).start()
    A[...] = jnp.zeros_like(A)
    B[...] = jnp.zeros_like(B)
    for r in range(2):
        xcopy(r, True).wait()

    def run(upd, wacc, src, dst):
        def s1(i, p):
            stage1(half, first + i * TR, p, X, VF, C, XS, YC, upd, wacc, src, dst)
        def s2(i, p):
            stage2(half, first + i * TR, p, C, XS, A, B, dst)
        if not wacc:
            lax.fori_loop(0, nt, lambda i, c: (s1(i, 0), c)[1], 0)
            return
        s1(0, 0)
        def body(i, c):
            p = lax.rem(i, 2)
            s2(i - 1, 1 - p)
            s1(i, p)
            return c
        lax.fori_loop(1, nt, body, 0)
        s2(nt - 1, (nt - 1) % 2)

    for r in range(2):
        vcopy(6, 0, r).start()
    for r in range(2):
        vcopy(7, 1, r).wait()
    run(False, True, 0, 1)
    make_y(tq[7], A, B, YC)
    def panel(k, c):
        q = 6 - k
        slot = lax.rem(q, 2)
        @pl.when(q > 0)
        def _():
            for r in range(2):
                vcopy(q - 1, 1 - slot, r).start()
        for r in range(2):
            vcopy(q, slot, r).wait()
        run(True, True, 1 - slot, slot)
        make_y(tq[q], A, B, YC)
        return c
    lax.fori_loop(0, 7, panel, 0)
    run(True, False, 0, 1)
    for r in range(2):
        xcopy(r, False).start()
    for r in range(2):
        xcopy(r, False).wait()

def group_call(t, vt, tq, x):
    nrow, ncol = x.shape
    any_spec = pl.BlockSpec(memory_space=pl.ANY)
    flops = 8 * 2 * 2 * 6 * 128 * ncol * (nrow - 2 * TR * t)
    return pl.pallas_call(
        functools.partial(group_kernel, t),
        out_shape=jax.ShapeDtypeStruct(x.shape, F32),
        in_specs=[any_spec, pl.BlockSpec(memory_space=pltpu.VMEM), any_spec],
        out_specs=any_spec,
        scratch_shapes=[
            pltpu.VMEM((nrow, ncol), F32),
            pltpu.VMEM((2, nrow, 128), F32),
            pltpu.VMEM((2, 2, nrow, 256), BF),
            pltpu.VMEM((2, 3, 2 * TR, ncol), BF),
            pltpu.VMEM((3, 256, ncol), BF),
            pltpu.VMEM((256, ncol), F32),
            pltpu.VMEM((128, ncol), F32),
            pltpu.SemaphoreType.DMA((2, 2)),
            pltpu.SemaphoreType.DMA((2,)),
        ],
        input_output_aliases={2: 0},
        compiler_params=pltpu.CompilerParams(vmem_limit_bytes=60 * 1024 * 1024),
        cost_estimate=pl.CostEstimate(flops=flops, bytes_accessed=4 * (nrow * 128 * 8 + 2 * nrow * ncol), transcendentals=0),
        name=f"group{t}",
    )(vt, tq, x)


def solution(mesh):
    def local_apply(v_loc, t_loc, z_loc):
        num_local = t_loc.shape[0]
        t_all = lax.all_gather(t_loc, "col")
        x = z_loc
        vs = {}
        for t in range(num_local - 1, -1, -1):
            vs[t] = lax.all_gather(v_loc[TR * t:, t * 128:(t + 1) * 128], ("row", "col"))
        for t in range(num_local - 1, -1, -1):
            x = group_call(t, vs[t], t_all[:, t], x)
        return x

    return jax.shard_map(
        local_apply,
        mesh=mesh,
        in_specs=(jax.sharding.PartitionSpec("row", "col"), jax.sharding.PartitionSpec("col", None, None), jax.sharding.PartitionSpec(None, ("row", "col"))),
        out_specs=jax.sharding.PartitionSpec(None, ("row", "col")),
        check_vma=False,
    )
```

```python
import jax
import jax.numpy as jnp
from jax import lax
from jax.experimental import pallas as pl
from jax.experimental.pallas import tpu as pltpu
from jax.sharding import PartitionSpec as P

BF = jnp.bfloat16
F32 = jnp.float32
TN = (((0,), (0,)), ((), ()))
TR = 512
BW = 128
NT = 8
NPAIR = 4 * NT
NSLOT = 2 * NT * (NT + 1)
MESH = pl.DeviceIdType.MESH
HOP_LAG = 12
DONE_LAG = 52


def split3(v):
    h = v.astype(BF)
    r = v - h.astype(F32)
    m = r.astype(BF)
    l = (r - m.astype(F32)).astype(BF)
    return h, m, l


def mm(a, b):
    return jnp.dot(a, b, preferred_element_type=F32)


def mmt(a, b):
    return lax.dot_general(a, b, TN, preferred_element_type=F32)


def stage1(half, off, p, X, VF, C, XS, YC, wacc, src, dst):
    for r in range(2):
        rows = pl.ds(pl.multiple_of(r * half + off, TR), TR)
        x = X[rows, :]
        x = x - (mm(C[src, 0, rows, :], YC[0]) + mm(C[src, 0, rows, :], YC[1]) + mm(C[src, 1, rows, :], YC[2]))
        X[rows, :] = x
        if wacc:
            prow = pl.ds(r * TR, TR)
            xh, xm, xl = split3(x)
            XS[p, 0, prow, :] = xh
            XS[p, 1, prow, :] = xm
            XS[p, 2, prow, :] = xl
            vh, vm, vl = split3(VF[dst, rows, :])
            C[dst, 0, rows, :BW] = vh
            C[dst, 0, rows, BW:] = vm
            C[dst, 1, rows, :BW] = vh
            C[dst, 1, rows, BW:] = vl


def stage2(half, off, p, C, XS, A, B, dst):
    a = A[...]
    b = B[...]
    for r in range(2):
        rows = pl.ds(pl.multiple_of(r * half + off, TR), TR)
        prow = pl.ds(r * TR, TR)
        n1 = C[dst, 0, rows, :]
        a += mmt(n1, XS[p, 0, prow, :]) + mmt(n1, XS[p, 1, prow, :])
        b += mmt(C[dst, 1, rows, BW:], XS[p, 0, prow, :]) + mmt(n1[:, :BW], XS[p, 2, prow, :])
    A[...] = a
    B[...] = b


def make_y(tq, A, B, YC):
    w = A[:BW, :] + A[BW:, :] + B[...]
    th, tm, tl = split3(tq)
    wh, wm, wl = split3(w)
    t1 = jnp.concatenate([th, tm], axis=1)
    t2 = jnp.concatenate([th, tl], axis=1)
    y = (
        mm(t1, jnp.concatenate([wh, wh], axis=0))
        + mm(t1, jnp.concatenate([wm, wm], axis=0))
        + mm(t2, jnp.concatenate([wl, wh], axis=0))
    )
    yh, ym, yl = split3(y)
    YC[0] = jnp.concatenate([yh, yh], axis=0)
    YC[1] = jnp.concatenate([ym, ym], axis=0)
    YC[2] = jnp.concatenate([yl, yh], axis=0)
    A[...] = jnp.zeros_like(A)
    B[...] = jnp.zeros_like(B)


def kernel(v_loc, head, x_in, x_out, G, X, VF, C, XS, YC, A, B, TQ, recv, sib, vsem, xsem, send):
    half = X.shape[0] // 2
    z0 = lax.axis_index("row")
    c0 = lax.axis_index("col")
    y0 = c0 // 4
    x0 = (c0 // 2) % 2
    k0 = c0 % 2
    me = (x0, y0, z0)
    partner = (z0, c0 + 1 - 2 * k0)
    peers = ((z0, c0 + 2 - 4 * x0), (z0, c0 + 4 - 8 * y0), (1 - z0, c0))

    def pair_of(pr):
        w = pr // 4 + 1
        return w, NT - w, 3 - pr % 4

    def decode(s):
        w = 1
        for v in range(1, NT):
            w = w + (s >= 2 * v * (v + 1)).astype(jnp.int32)
        rem = s - 2 * w * (w - 1)
        back = (rem >= w).astype(jnp.int32) + (rem >= 2 * w).astype(jnp.int32) + (rem >= 3 * w).astype(jnp.int32)
        return w, 3 - back, rem - back * w

    def slot_of(w, p, i):
        return 2 * w * (w - 1) + (3 - p) * w + i

    def xcopy_in():
        return pltpu.make_async_copy(x_in, X, xsem.at[0, 0])

    xcopy_in().start()
    barrier = pltpu.get_barrier_semaphore()
    for dev in (*peers, partner):
        pl.semaphore_signal(barrier, inc=1, device_id=dev, device_id_type=MESH)
    pl.semaphore_wait(barrier, 4)

    def push(src, s, r, dev, sem_arr, which):
        pltpu.make_async_remote_copy(
            src_ref=src,
            dst_ref=G.at[s, k0, r],
            send_sem=send.at[which],
            recv_sem=sem_arr.at[s, r],
            device_id=dev,
            device_id_type=MESH,
        ).start()

    rows3 = (z0, z0, 1 - z0)
    cols3 = (c0 + 2 - 4 * x0, c0 + 4 - 8 * y0, c0)

    def turn(k, v, j):
        a, b, c = v[j % 3], v[(j + 1) % 3], v[(j + 2) % 3]
        return jnp.where(k == 0, a, jnp.where(k == 1, b, c))

    def chunk(t, i):
        rows = pl.ds(pl.multiple_of((t + i) * TR, TR), TR)
        return v_loc.at[rows, pl.ds(pl.multiple_of(t * BW, BW), BW)]

    def hop(s, depth):
        w, p, i = decode(s)
        k = (i + w) % 3
        xy = ((x0 + p) % 2, (y0 + p // 2) % 2)
        for r in range(2):
            bits = (xy[0], xy[1], (z0 + r) % 2)
            e0, e1, e2 = turn(k, bits, 0), turn(k, bits, 1), turn(k, bits, 2)
            far = e1 + e2
            mine = jnp.where(e0 + far == 0, 0, 2 - e0 + far)

            @pl.when(mine == depth)
            def _():
                to = [(turn(k, rows3, j), turn(k, cols3, j)) for j in range(3)]

                @pl.when(mine == 0)
                def _():
                    @pl.when(i == 0)
                    def _():
                        o = head.at[w - 1]
                        push(o, s, r, to[0], recv, 0)
                        push(o, s, r, partner, sib, 1)

                    @pl.when(i > 0)
                    def _():
                        o = chunk(NT - w, i)
                        push(o, s, r, to[0], recv, 0)
                        push(o, s, r, partner, sib, 1)

                @pl.when(mine > 0)
                def _():
                    g = G.at[s, k0, r]
                    pltpu.make_async_copy(g, g, recv.at[s, r]).wait()

                    @pl.when(e0 == 1)
                    def _():
                        @pl.when(far == 0)
                        def _():
                            push(g, s, r, to[1], recv, 0)

                        @pl.when(e2 == 0)
                        def _():
                            push(g, s, r, to[2], recv, 0)

                        @pl.when(far > 0)
                        def _():
                            push(g, s, r, to[0], recv, 0)

                    push(g, s, r, partner, sib, 1)

    def tick(tau):
        def one(h, carry):
            s = tau - jnp.where(h == 0, 0, 1 + HOP_LAG * h)

            @pl.when(jnp.logical_and(s >= 0, s < NSLOT))
            def _():
                hop(s, h)

            return carry

        lax.fori_loop(0, 5, one, 0)

    def ticks(lo, hi):
        def one(tau, carry):
            tick(tau)
            return carry

        lax.fori_loop(lo, hi, one, 0)

    def start_of(n):
        w, t, p = pair_of(n // 2)
        return slot_of(w, p, 0) + w + DONE_LAG + (n % 2) * (w // 2)

    def await_sibling(pr):
        w, t, p = pair_of(pr)

        def one(i, carry):
            for r in range(2):
                g = G.at[slot_of(w, p, i), 1 - k0, r]
                pltpu.make_async_copy(g, g, sib.at[slot_of(w, p, i), r]).wait()
            return carry

        lax.fori_loop(0, w, one, 0)

    def load(n, slot, wait):
        pr = n // 2
        b = 1 - n % 2
        w, t, p = pair_of(pr)

        def one(i, carry):
            for r in range(2):
                dst = VF.at[slot, pl.ds(pl.multiple_of(r * half + (t + i) * TR, TR), TR), :]
                if wait:
                    pltpu.make_async_copy(G.at[0, 0, 0], dst, vsem.at[slot, i, r]).wait()
                else:
                    is_own = jnp.logical_and(jnp.logical_and(z0 == r, b == k0), c0 // 2 == p)

                    @pl.when(jnp.logical_and(is_own, i == 0))
                    def _():
                        pltpu.make_async_copy(head.at[w - 1], dst, vsem.at[slot, i, r]).start()

                    @pl.when(jnp.logical_and(is_own, i > 0))
                    def _():
                        pltpu.make_async_copy(chunk(t, i), dst, vsem.at[slot, i, r]).start()

                    @pl.when(jnp.logical_not(is_own))
                    def _():
                        pltpu.make_async_copy(G.at[slot_of(w, p, i), b, r], dst, vsem.at[slot, i, r]).start()
            return carry

        lax.fori_loop(0, w, one, 0)

    def compute(n):
        pr = n // 2
        b = 1 - n % 2
        dst = n % 2
        src = 1 - dst
        w, t, p = pair_of(pr)
        first = t * TR

        @pl.when(n % 8 == 0)
        def _():
            for r in range(2):
                rows = pl.ds(pl.multiple_of(r * half + first, TR), TR)
                C[src, :, rows, :] = jnp.zeros((2, TR, 2 * BW), BF)

        drow = pl.ds(pl.multiple_of(b * half + first + BW * p, BW), BW)
        blk = VF[dst, drow, :]
        ri = lax.broadcasted_iota(jnp.int32, (BW, BW), 0)
        ci = lax.broadcasted_iota(jnp.int32, (BW, BW), 1)
        TQ[...] = jnp.where(ci >= ri, blk, 0.0)
        VF[dst, drow, :] = jnp.where(ri > ci, blk, jnp.where(ri == ci, 1.0, 0.0))

        stage1(half, first, 0, X, VF, C, XS, YC, True, src, dst)
        now = start_of(n)

        def body(i, carry):
            q = lax.rem(i, 2)
            stage2(half, first + (i - 1) * TR, 1 - q, C, XS, A, B, dst)
            stage1(half, first + i * TR, q, X, VF, C, XS, YC, True, src, dst)

            @pl.when(q == 1)
            def _():
                tick(now + i // 2)

            return carry

        lax.fori_loop(1, w, body, 0)

        @pl.when(n < 2 * NPAIR - 1)
        def _():
            ticks(now + w // 2, start_of(n + 1))

            @pl.when(n % 2 == 1)
            def _():
                await_sibling(pr + 1)

            load(n + 1, src, False)

        stage2(half, first + (w - 1) * TR, lax.rem(w - 1, 2), C, XS, A, B, dst)
        make_y(TQ[...], A, B, YC)

    A[...] = jnp.zeros_like(A)
    B[...] = jnp.zeros_like(B)
    YC[...] = jnp.zeros_like(YC)

    ticks(0, start_of(0))
    await_sibling(0)
    load(0, 0, False)
    xcopy_in().wait()

    def panel(n, carry):
        load(n, n % 2, True)
        compute(n)
        return carry

    lax.fori_loop(0, 2 * NPAIR, panel, 0)

    def xcopy_out(i, r):
        rows = pl.ds(pl.multiple_of(r * half + i * TR, TR), TR)
        return pltpu.make_async_copy(X.at[rows, :], x_out.at[rows, :], xsem.at[i, r])

    def finish(i, carry):
        stage1(half, i * TR, 0, X, VF, C, XS, YC, False, 1, 0)
        for r in range(2):
            xcopy_out(i, r).start()
        return carry

    lax.fori_loop(0, NT, finish, 0)

    def drain(i, carry):
        for r in range(2):
            xcopy_out(i, r).wait()
        return carry

    lax.fori_loop(0, NT, drain, 0)
    nown = NT * (NT + 1) // 2
    sent = G.at[pl.ds(0, 7 * nown // 4)]
    pltpu.make_async_copy(sent, sent, send.at[0]).wait()
    given = G.at[pl.ds(0, 8 * nown // 4)]
    pltpu.make_async_copy(given, given, send.at[1]).wait()


def pack_heads(v_loc, t_loc):
    r = lax.axis_index("row")
    q = lax.axis_index("col")
    off = BW * ((q - r) // 2)
    has = q % 2 == r
    ri = lax.broadcasted_iota(jnp.int32, (NT, TR, BW), 1) - off
    ci = lax.broadcasted_iota(jnp.int32, (NT, TR, BW), 2)
    mask = has & (ri >= 0) & (ri < BW) & (ci >= ri)
    heads = jnp.stack([v_loc[t * TR : (t + 1) * TR, t * BW : (t + 1) * BW] for t in range(NT - 1, -1, -1)])
    t_pad = jnp.pad(t_loc[::-1], ((0, 0), (TR, TR - BW), (0, 0)))
    return jnp.where(mask, lax.dynamic_slice_in_dim(t_pad, TR - off, TR, axis=1), heads)


def solution(mesh):
    def local_apply(v_loc, t_loc, z_loc):
        nrow, ncol = z_loc.shape
        head = pack_heads(v_loc, t_loc)
        any_spec = pl.BlockSpec(memory_space=pl.ANY)
        x, _ = pl.pallas_call(
            kernel,
            out_shape=(
                jax.ShapeDtypeStruct((nrow, ncol), F32),
                jax.ShapeDtypeStruct((NSLOT, 2, 2, TR, BW), F32),
            ),
            in_specs=[any_spec, any_spec, any_spec],
            out_specs=(any_spec, any_spec),
            scratch_shapes=[
                pltpu.VMEM((nrow, ncol), F32),
                pltpu.VMEM((2, nrow, BW), F32),
                pltpu.VMEM((2, 2, nrow, 2 * BW), BF),
                pltpu.VMEM((2, 3, 2 * TR, ncol), BF),
                pltpu.VMEM((3, 2 * BW, ncol), BF),
                pltpu.VMEM((2 * BW, ncol), F32),
                pltpu.VMEM((BW, ncol), F32),
                pltpu.VMEM((BW, BW), F32),
                pltpu.SemaphoreType.DMA((NSLOT, 2)),
                pltpu.SemaphoreType.DMA((NSLOT, 2)),
                pltpu.SemaphoreType.DMA((2, NT, 2)),
                pltpu.SemaphoreType.DMA((NT, 2)),
                pltpu.SemaphoreType.DMA((2,)),
            ],
            compiler_params=pltpu.CompilerParams(
                collective_id=0, has_side_effects=True, vmem_limit_bytes=60 * 1024 * 1024
            ),
            name="back_transform",
        )(v_loc, head, z_loc)
        return x

    return jax.shard_map(
        local_apply,
        mesh=mesh,
        in_specs=(P("row", "col"), P("col", None, None), P(None, ("row", "col"))),
        out_specs=P(None, ("row", "col")),
        check_vma=False,
    )
```

```python
import jax
import jax.numpy as jnp
from jax import lax
from jax.experimental import pallas as pl
from jax.experimental.pallas import tpu as pltpu
from jax.sharding import PartitionSpec as P

BF = jnp.bfloat16
F32 = jnp.float32
TN = (((0,), (0,)), ((), ()))
TR = 512
BW = 128
NT = 8
NPAIR = 4 * NT
NSLOT = 2 * NT * (NT + 1)
MESH = pl.DeviceIdType.MESH
LAGS = ((3, 4), (5, 7), (NT, 10))


def split3(v):
    h = v.astype(BF)
    r = v - h.astype(F32)
    m = r.astype(BF)
    l = (r - m.astype(F32)).astype(BF)
    return h, m, l


def mm(a, b):
    return jnp.dot(a, b, preferred_element_type=F32)


def mmt(a, b):
    return lax.dot_general(a, b, TN, preferred_element_type=F32)


def stage1(half, off, p, X, VF, C, XS, YC, wacc, src, dst):
    for r in range(2):
        rows = pl.ds(pl.multiple_of(r * half + off, TR), TR)
        x = X[rows, :]
        x = x - (mm(C[src, 0, rows, :], YC[0]) + mm(C[src, 0, rows, :], YC[1]) + mm(C[src, 1, rows, :], YC[2]))
        X[rows, :] = x
        if wacc:
            prow = pl.ds(r * TR, TR)
            xh, xm, xl = split3(x)
            XS[p, 0, prow, :] = xh
            XS[p, 1, prow, :] = xm
            XS[p, 2, prow, :] = xl
            vh, vm, vl = split3(VF[dst, rows, :])
            C[dst, 0, rows, :BW] = vh
            C[dst, 0, rows, BW:] = vm
            C[dst, 1, rows, :BW] = vh
            C[dst, 1, rows, BW:] = vl


def stage2(half, off, p, C, XS, A, B, dst):
    a = A[...]
    b = B[...]
    for r in range(2):
        rows = pl.ds(pl.multiple_of(r * half + off, TR), TR)
        prow = pl.ds(r * TR, TR)
        n1 = C[dst, 0, rows, :]
        a += mmt(n1, XS[p, 0, prow, :]) + mmt(n1, XS[p, 1, prow, :])
        b += mmt(C[dst, 1, rows, BW:], XS[p, 0, prow, :]) + mmt(n1[:, :BW], XS[p, 2, prow, :])
    A[...] = a
    B[...] = b


def make_y(tq, A, B, YC):
    w = A[:BW, :] + A[BW:, :] + B[...]
    th, tm, tl = split3(tq)
    wh, wm, wl = split3(w)
    t1 = jnp.concatenate([th, tm], axis=1)
    t2 = jnp.concatenate([th, tl], axis=1)
    y = (
        mm(t1, jnp.concatenate([wh, wh], axis=0))
        + mm(t1, jnp.concatenate([wm, wm], axis=0))
        + mm(t2, jnp.concatenate([wl, wh], axis=0))
    )
    yh, ym, yl = split3(y)
    YC[0] = jnp.concatenate([yh, yh], axis=0)
    YC[1] = jnp.concatenate([ym, ym], axis=0)
    YC[2] = jnp.concatenate([yl, yh], axis=0)
    A[...] = jnp.zeros_like(A)
    B[...] = jnp.zeros_like(B)


def kernel(v_loc, head, x_in, x_out, G, X, VF, C, XS, YC, A, B, TQ, recv, sib, vsem, xsem, send):
    half = X.shape[0] // 2
    z0 = lax.axis_index("row")
    c0 = lax.axis_index("col")
    y0 = c0 // 4
    x0 = (c0 // 2) % 2
    k0 = c0 % 2
    me = (x0, y0, z0)
    partner = (z0, c0 + 1 - 2 * k0)
    peers = ((z0, c0 + 2 - 4 * x0), (z0, c0 + 4 - 8 * y0), (1 - z0, c0))

    def pair_of(pr):
        w = pr // 4 + 1
        return w, NT - w, 3 - pr % 4

    def decode(s):
        w = 1
        for v in range(1, NT):
            w = w + (s >= 2 * v * (v + 1)).astype(jnp.int32)
        rem = s - 2 * w * (w - 1)
        back = (rem >= w).astype(jnp.int32) + (rem >= 2 * w).astype(jnp.int32) + (rem >= 3 * w).astype(jnp.int32)
        return w, 3 - back, rem - back * w

    def slot_of(w, p, i):
        return 2 * w * (w - 1) + (3 - p) * w + i

    def xcopy_in():
        return pltpu.make_async_copy(x_in, X, xsem.at[0, 0])

    xcopy_in().start()
    barrier = pltpu.get_barrier_semaphore()
    for dev in (*peers, partner):
        pl.semaphore_signal(barrier, inc=1, device_id=dev, device_id_type=MESH)
    pl.semaphore_wait(barrier, 4)

    def push(src, s, r, dev, sem_arr, which):
        pltpu.make_async_remote_copy(
            src_ref=src,
            dst_ref=G.at[s, k0, r],
            send_sem=send.at[which],
            recv_sem=sem_arr.at[s, r],
            device_id=dev,
            device_id_type=MESH,
        ).start()

    rows3 = (z0, z0, 1 - z0)
    cols3 = (c0 + 2 - 4 * x0, c0 + 4 - 8 * y0, c0)

    def turn(k, v, j):
        a, b, c = v[j % 3], v[(j + 1) % 3], v[(j + 2) % 3]
        return jnp.where(k == 0, a, jnp.where(k == 1, b, c))

    def chunk(t, i):
        rows = pl.ds(pl.multiple_of((t + i) * TR, TR), TR)
        return v_loc.at[rows, pl.ds(pl.multiple_of(t * BW, BW), BW)]

    def hop(s, depth):
        w, p, i = decode(s)
        k = (i + w) % 3
        xy = ((x0 + p) % 2, (y0 + p // 2) % 2)
        for r in range(2):
            bits = (xy[0], xy[1], (z0 + r) % 2)
            e0, e1, e2 = turn(k, bits, 0), turn(k, bits, 1), turn(k, bits, 2)
            far = e1 + e2
            mine = jnp.where(e0 + far == 0, 0, 2 - e0 + far)

            @pl.when(mine == depth)
            def _():
                to = [(turn(k, rows3, j), turn(k, cols3, j)) for j in range(3)]

                @pl.when(mine == 0)
                def _():
                    @pl.when(i == 0)
                    def _():
                        o = head.at[w - 1]
                        push(o, s, r, to[0], recv, 0)
                        push(o, s, r, partner, sib, 1)

                    @pl.when(i > 0)
                    def _():
                        o = chunk(NT - w, i)
                        push(o, s, r, to[0], recv, 0)
                        push(o, s, r, partner, sib, 1)

                @pl.when(mine > 0)
                def _():
                    g = G.at[s, k0, r]
                    pltpu.make_async_copy(g, g, recv.at[s, r]).wait()

                    @pl.when(e0 == 1)
                    def _():
                        @pl.when(far == 0)
                        def _():
                            push(g, s, r, to[1], recv, 0)

                        @pl.when(e2 == 0)
                        def _():
                            push(g, s, r, to[2], recv, 0)

                        @pl.when(far > 0)
                        def _():
                            push(g, s, r, to[0], recv, 0)

                    push(g, s, r, partner, sib, 1)

    def tick(tau):
        def one(h, carry):
            s = jnp.int32(-1)
            for j, (top, lag) in enumerate(LAGS):
                bottom = LAGS[j - 1][0] if j else 0
                cand = tau - 1 - lag * h
                fits = jnp.logical_and(cand >= 2 * bottom * (bottom + 1), cand < 2 * top * (top + 1))
                s = jnp.where(fits, cand, s)
            s = jnp.where(h == 0, tau, s)

            @pl.when(jnp.logical_and(s >= 0, s < NSLOT))
            def _():
                hop(s, h)

            return carry

        lax.fori_loop(0, 5, one, 0)

    def ticks(lo, hi):
        def one(tau, carry):
            tick(tau)
            return carry

        lax.fori_loop(lo, hi, one, 0)

    def start_of(n):
        w, t, p = pair_of(n // 2)
        done = jnp.int32(0)
        for top, lag in LAGS[::-1]:
            done = jnp.where(w <= top, 4 * lag + 4, done)
        return slot_of(w, p, 0) + w + done + (n % 2) * (w // 2)

    def await_sibling(pr):
        w, t, p = pair_of(pr)

        def one(i, carry):
            for r in range(2):
                g = G.at[slot_of(w, p, i), 1 - k0, r]
                pltpu.make_async_copy(g, g, sib.at[slot_of(w, p, i), r]).wait()
            return carry

        lax.fori_loop(0, w, one, 0)

    def load(n, slot, wait):
        pr = n // 2
        b = 1 - n % 2
        w, t, p = pair_of(pr)

        def one(i, carry):
            for r in range(2):
                dst = VF.at[slot, pl.ds(pl.multiple_of(r * half + (t + i) * TR, TR), TR), :]
                if wait:
                    pltpu.make_async_copy(G.at[0, 0, 0], dst, vsem.at[slot, i, r]).wait()
                else:
                    is_own = jnp.logical_and(jnp.logical_and(z0 == r, b == k0), c0 // 2 == p)

                    @pl.when(jnp.logical_and(is_own, i == 0))
                    def _():
                        pltpu.make_async_copy(head.at[w - 1], dst, vsem.at[slot, i, r]).start()

                    @pl.when(jnp.logical_and(is_own, i > 0))
                    def _():
                        pltpu.make_async_copy(chunk(t, i), dst, vsem.at[slot, i, r]).start()

                    @pl.when(jnp.logical_not(is_own))
                    def _():
                        pltpu.make_async_copy(G.at[slot_of(w, p, i), b, r], dst, vsem.at[slot, i, r]).start()
            return carry

        lax.fori_loop(0, w, one, 0)

    def compute(n):
        pr = n // 2
        b = 1 - n % 2
        dst = n % 2
        src = 1 - dst
        w, t, p = pair_of(pr)
        first = t * TR

        @pl.when(n % 8 == 0)
        def _():
            for r in range(2):
                rows = pl.ds(pl.multiple_of(r * half + first, TR), TR)
                C[src, :, rows, :] = jnp.zeros((2, TR, 2 * BW), BF)

        drow = pl.ds(pl.multiple_of(b * half + first + BW * p, BW), BW)
        blk = VF[dst, drow, :]
        ri = lax.broadcasted_iota(jnp.int32, (BW, BW), 0)
        ci = lax.broadcasted_iota(jnp.int32, (BW, BW), 1)
        TQ[...] = jnp.where(ci >= ri, blk, 0.0)
        VF[dst, drow, :] = jnp.where(ri > ci, blk, jnp.where(ri == ci, 1.0, 0.0))

        stage1(half, first, 0, X, VF, C, XS, YC, True, src, dst)
        now = start_of(n)

        def body(i, carry):
            q = lax.rem(i, 2)
            stage2(half, first + (i - 1) * TR, 1 - q, C, XS, A, B, dst)
            stage1(half, first + i * TR, q, X, VF, C, XS, YC, True, src, dst)

            @pl.when(q == 1)
            def _():
                tick(now + i // 2)

            return carry

        lax.fori_loop(1, w, body, 0)

        @pl.when(n < 2 * NPAIR - 1)
        def _():
            ticks(now + w // 2, start_of(n + 1))

            @pl.when(n % 2 == 1)
            def _():
                await_sibling(pr + 1)

            load(n + 1, src, False)

        stage2(half, first + (w - 1) * TR, lax.rem(w - 1, 2), C, XS, A, B, dst)
        make_y(TQ[...], A, B, YC)

    A[...] = jnp.zeros_like(A)
    B[...] = jnp.zeros_like(B)
    YC[...] = jnp.zeros_like(YC)

    ticks(0, start_of(0))
    await_sibling(0)
    load(0, 0, False)
    xcopy_in().wait()

    def panel(n, carry):
        load(n, n % 2, True)
        compute(n)
        return carry

    lax.fori_loop(0, 2 * NPAIR, panel, 0)

    def xcopy_out(i, r):
        rows = pl.ds(pl.multiple_of(r * half + i * TR, TR), TR)
        return pltpu.make_async_copy(X.at[rows, :], x_out.at[rows, :], xsem.at[i, r])

    def finish(i, carry):
        stage1(half, i * TR, 0, X, VF, C, XS, YC, False, 1, 0)
        for r in range(2):
            xcopy_out(i, r).start()
        return carry

    lax.fori_loop(0, NT, finish, 0)

    def drain(i, carry):
        for r in range(2):
            xcopy_out(i, r).wait()
        return carry

    lax.fori_loop(0, NT, drain, 0)
    nown = NT * (NT + 1) // 2
    sent = G.at[pl.ds(0, 7 * nown // 4)]
    pltpu.make_async_copy(sent, sent, send.at[0]).wait()
    given = G.at[pl.ds(0, 8 * nown // 4)]
    pltpu.make_async_copy(given, given, send.at[1]).wait()


def pack_heads(v_loc, t_loc):
    r = lax.axis_index("row")
    q = lax.axis_index("col")
    off = BW * ((q - r) // 2)
    has = q % 2 == r
    ri = lax.broadcasted_iota(jnp.int32, (NT, TR, BW), 1) - off
    ci = lax.broadcasted_iota(jnp.int32, (NT, TR, BW), 2)
    mask = has & (ri >= 0) & (ri < BW) & (ci >= ri)
    heads = jnp.stack([v_loc[t * TR : (t + 1) * TR, t * BW : (t + 1) * BW] for t in range(NT - 1, -1, -1)])
    t_pad = jnp.pad(t_loc[::-1], ((0, 0), (TR, TR - BW), (0, 0)))
    return jnp.where(mask, lax.dynamic_slice_in_dim(t_pad, TR - off, TR, axis=1), heads)


def solution(mesh):
    def local_apply(v_loc, t_loc, z_loc):
        nrow, ncol = z_loc.shape
        head = pack_heads(v_loc, t_loc)
        any_spec = pl.BlockSpec(memory_space=pl.ANY)
        x, _ = pl.pallas_call(
            kernel,
            out_shape=(
                jax.ShapeDtypeStruct((nrow, ncol), F32),
                jax.ShapeDtypeStruct((NSLOT, 2, 2, TR, BW), F32),
            ),
            in_specs=[any_spec, any_spec, any_spec],
            out_specs=(any_spec, any_spec),
            scratch_shapes=[
                pltpu.VMEM((nrow, ncol), F32),
                pltpu.VMEM((2, nrow, BW), F32),
                pltpu.VMEM((2, 2, nrow, 2 * BW), BF),
                pltpu.VMEM((2, 3, 2 * TR, ncol), BF),
                pltpu.VMEM((3, 2 * BW, ncol), BF),
                pltpu.VMEM((2 * BW, ncol), F32),
                pltpu.VMEM((BW, ncol), F32),
                pltpu.VMEM((BW, BW), F32),
                pltpu.SemaphoreType.DMA((NSLOT, 2)),
                pltpu.SemaphoreType.DMA((NSLOT, 2)),
                pltpu.SemaphoreType.DMA((2, NT, 2)),
                pltpu.SemaphoreType.DMA((NT, 2)),
                pltpu.SemaphoreType.DMA((2,)),
            ],
            compiler_params=pltpu.CompilerParams(
                collective_id=0, has_side_effects=True, vmem_limit_bytes=60 * 1024 * 1024
            ),
            name="back_transform",
        )(v_loc, head, z_loc)
        return x

    return jax.shard_map(
        local_apply,
        mesh=mesh,
        in_specs=(P("row", "col"), P("col", None, None), P(None, ("row", "col"))),
        out_specs=P(None, ("row", "col")),
        check_vma=False,
    )
```
